32 devices in a mesh: expert: 16 (over z, y, x), tensor: 2 (over core).
Axes of the slice: x: 2, y: 2, z: 4, core: 2. Of those that a mesh axis runs over, the one named last changes fastest.
Arguments:
- tokens: bfloat16 [1024, 5120], P('expert', 'tensor'), may hold values from -6 to 6
- w_gate: bfloat16 [16, 5120, 1536], P('expert', None, 'tensor'), may hold values from -0.078125 to 0.078125
- w_up: bfloat16 [16, 5120, 1536], P('expert', None, 'tensor'), may hold values from -0.078125 to 0.078125
- w_down: bfloat16 [16, 1536, 5120], P('expert', 'tensor'), may hold values from -0.15625 to 0.15625
- route_ids: int32 [1024, 6], P('expert'), may hold values from 0 to 15, all different within a row; in each aligned block of 64 rows (0 to 63, 64 to 127, ...) at most 36 rows name the same one
- route_weight: float32 [1024, 6], P('expert'), may hold values from 0.1 to 1
- live_count: int32 [16], P('expert'), may hold values from 32 to 64, as said below
- owner_slot: int32 [1024], P('expert'), may hold values from 0 to 63, as said below
Outputs:
- mixed: bfloat16 [1024, 5120], P('expert', 'tensor')
The draws below stay inside these ranges and needn't reach their ends.
Inputs may be any that keep to these rules, and one draw needn't show every extreme that they name: `route_ids`: each row names 6 different experts; among the 64 rows of one index of expert no expert is named by more than 36 rows, and in some index one expert is named by exactly 36. `live_count`: a multiple of 16; some index of expert has all 64 slots live. `owner_slot`: within the 64 rows of each index of expert, each of 0 to 63 once.
All inputs are finite; a program needn't handle non-finite values.
Results may differ from the reference program's by a relative error of at most 0.0057.
Values may be sent and summed in bfloat16 or wider, within the bound.
No kernel may reach another device: no remote copies, remote signals or barrier semaphores. Data moves between devices by JAX's collectives and lax.ppermute only.
A program may use at most 128 MiB of HBM per device.

```python
import math
import jax
import jax.numpy as jnp
import numpy as np
from jax import lax

D = 5120
FF = 1536
TOP = 6
TOK_DEV = 64
EXPERTS = 16
CAP = 36
TOKENS = 1024
N_EXPERT = 16


def draw_live_count(key, part):
    groups = TOKENS // TOK_DEV
    first_key, second_key = jax.random.split(jax.random.fold_in(key, 11))
    quarters = jax.random.randint(first_key, (groups,), 2, 5)
    counts = TOK_DEV * quarters // 4
    fullest = jax.random.randint(second_key, (), 0, groups)
    return jnp.where(jnp.arange(groups) == fullest, TOK_DEV, counts).astype(jnp.int32)


def draw_owner_slot(key, part):
    groups = TOKENS // TOK_DEV
    keys = jax.random.split(jax.random.fold_in(key, 23), groups)
    orders = jax.vmap(lambda single: jax.random.permutation(single, TOK_DEV))(keys)
    return orders.reshape(-1).astype(jnp.int32)


def block_levels(rng, extent, cuts, low, high):
    factor_of, own = 1.0, jax.random.fold_in(rng, 6)
    for axis_at, shards_of in cuts:
        heights = jnp.exp(jax.random.uniform(jax.random.fold_in(own, axis_at), (shards_of,), jnp.float32, low / len(cuts), high / len(cuts)))
        factor_of = factor_of * jnp.repeat(heights, extent[axis_at] // shards_of).reshape([-1 if axis == axis_at else 1 for axis in range(len(extent))])
    return factor_of


def shared_out(rng, own, number, rows, number_of, top, most, skew):
    order = jax.random.permutation(rng, number_of)
    crowded, common = shares(number_of, rows * top, most, skew, True), shares(number_of, rows * top, most, skew, False)
    places = jnp.arange(number_of)

    def named(lengths, rotation):
        used = int((lengths > 0).sum())
        fixed = max(1, used // 4)
        passed = fixed + (places - fixed + rotation * (used - fixed)) % max(1, number_of - fixed)
        return jnp.zeros((number_of,), jnp.int32).at[order[jnp.where(places < fixed, places, passed)]].set(jnp.asarray(lengths, jnp.int32))

    lengths = jnp.where(number % 4 == 0, named(crowded, number // 4), named(common, number - number // 4 - 1))
    mixed = jax.random.permutation(jax.random.fold_in(own, 3), number_of)
    source_of, sink = mixed[0:number_of // 2 * 2:2], mixed[1:number_of // 2 * 2:2]
    margin = jnp.minimum(lengths[source_of] - 1, most - lengths[sink]) // 2
    margin = jnp.where((source_of == order[0]) | (sink == order[0]) | (lengths[sink] == 0), 0, jnp.maximum(margin, 0))
    passed = jax.random.randint(jax.random.fold_in(own, 4), (number_of // 2,), 0, 1 << 20) % (margin + 1)
    lengths = lengths.at[source_of].add(-passed).at[sink].add(passed)
    labels = jnp.searchsorted(jnp.cumsum(lengths), jnp.arange(rows * top), side="right").astype(jnp.int32)
    grid = labels.reshape(top, rows).T
    grid = grid[jax.random.permutation(jax.random.fold_in(own, 1), rows)]
    rotation = jax.random.randint(jax.random.fold_in(own, 2), (rows, 1), 0, top)
    return jnp.take_along_axis(grid, (jnp.arange(top)[None, :] + rotation) % top, axis=1)


def shares(count, total, most, slope, full):
    weights = [(1 << 20) // math.isqrt(standing ** slope) + 1 for standing in range(1, count + 1)]
    largest = most if full else min(most, max(-(-total // count), total * weights[0] // sum(weights)))
    least = 1 if total - largest >= count - 1 else 0
    given, spare = [largest] + [least] * (count - 1), total - largest - least * (count - 1)
    while spare > 0:
        movable = [i for i in range(1, count) if given[i] < largest] or [i for i in range(1, count) if given[i] < most]
        mass, budget = sum([weights[i] for i in movable]), spare
        for i in movable:
            more = min(most - given[i], max(1, budget * weights[i] // mass), spare)
            given[i] = given[i] + more
            spare = spare - more
    return np.array(given)


def centred(key, extent, width, most, cuts=(), kind=jnp.bfloat16):
    factor_of = block_levels(key, extent, cuts, -0.22, 0.18) if cuts else 1.0
    values = jax.random.normal(key, extent, jnp.float32) * width * factor_of
    return jnp.minimum(jnp.maximum(values, -most), most).astype(kind)


def setup_inputs(seed: int = 0) -> dict:
    streams_of = jax.random.split(jax.random.key(seed), 9)
    tokens = centred(streams_of[0], (TOKENS, D), 1.0, 6.0, ((0, 16), (1, 2)))
    w_gate = centred(streams_of[1], (EXPERTS, D, FF), D ** -0.5, 0.078125, ((0, 16), (2, 2)))
    w_up = centred(streams_of[2], (EXPERTS, D, FF), D ** -0.5, 0.078125, ((0, 16), (2, 2)))
    w_down = centred(streams_of[3], (EXPERTS, FF, D), FF ** -0.5, 0.15625, ((0, 16), (1, 2)))
    route_ids_keys = jax.random.split(jax.random.fold_in(streams_of[4], 1), TOKENS // TOK_DEV)
    route_ids_turns = jax.random.permutation(jax.random.fold_in(streams_of[4], 3), TOKENS // TOK_DEV)
    route_ids = jax.vmap(lambda own, number: shared_out(jax.random.fold_in(streams_of[4], 2), own, number, TOK_DEV, EXPERTS, TOP, CAP, 2))(route_ids_keys, route_ids_turns).reshape((TOKENS, TOP))
    route_weight = jnp.clip(0.1 + 0.9 * jax.random.uniform(streams_of[5], (TOKENS, TOP), jnp.float32) ** block_levels(streams_of[5], (TOKENS, TOP), ((0, 16),), -0.2, 0.2), 0.1, 1.0)
    live_count = draw_live_count(jax.random.fold_in(streams_of[8], 71), 0)
    owner_slot = draw_owner_slot(jax.random.fold_in(streams_of[8], 71), 0)
    return dict(tokens=tokens, w_gate=w_gate, w_up=w_up, w_down=w_down, route_ids=route_ids, route_weight=route_weight, live_count=live_count, owner_slot=owner_slot)


def expert_rows(rows, gate_w, up_w, down_w):
    gate = jnp.dot(rows, gate_w, preferred_element_type=jnp.float32)
    up = jnp.dot(rows, up_w, preferred_element_type=jnp.float32)
    hidden = (jax.nn.silu(gate) * up).astype(jnp.bfloat16)
    return jnp.dot(hidden, down_w, preferred_element_type=jnp.float32).astype(jnp.bfloat16)


def reference(tokens, w_gate, w_up, w_down, route_ids, route_weight, live_count, owner_slot):
    slot_index = jnp.arange(TOKENS, dtype=jnp.int32) % TOK_DEV
    live = slot_index < jnp.repeat(live_count, TOK_DEV)
    flat_expert = route_ids.reshape(-1)
    flat_token = jnp.repeat(jnp.arange(TOKENS, dtype=jnp.int32), TOP)
    flat_live = jnp.repeat(live, TOP)
    flat_weight = route_weight.reshape(-1)
    ordering = jnp.argsort(flat_expert, stable=True).astype(jnp.int32)
    per_expert = jnp.sum((flat_expert[:, None] == jnp.arange(EXPERTS, dtype=jnp.int32)[None, :]).astype(jnp.int32), 0).astype(jnp.int32)
    starts = (jnp.cumsum(per_expert) - per_expert).astype(jnp.int32)
    limit = N_EXPERT * CAP
    padded = jnp.concatenate([ordering, jnp.zeros((limit,), jnp.int32)])

    def one_expert(total, expert_id):
        pick = lax.dynamic_slice_in_dim(padded, starts[expert_id], limit)
        valid = (jnp.arange(limit, dtype=jnp.int32) < per_expert[expert_id]) & flat_live[pick]
        token_id = flat_token[pick]
        result = expert_rows(tokens[token_id], w_gate[expert_id], w_up[expert_id], w_down[expert_id])
        weight = jnp.where(valid, flat_weight[pick], jnp.float32(0.0))
        total = total.at[token_id].add(weight[:, None] * result.astype(jnp.float32))
        return total, None

    combined, _ = lax.scan(one_expert, jnp.zeros((TOKENS, D), jnp.float32), jnp.arange(EXPERTS, dtype=jnp.int32))
    rows_index = (jnp.arange(TOKENS, dtype=jnp.int32) // TOK_DEV) * TOK_DEV + owner_slot
    return combined[rows_index].astype(jnp.bfloat16)
```

```python
import jax
import jax.numpy as jnp
from jax import lax
from jax.sharding import PartitionSpec as P

CHUNKS = 2
BOTH = ("expert", "tensor")


def exchange_body(tokens, w_gate, w_up, w_down, route_ids, route_weight, live_count, owner_slot):
    tok_dev, top = route_ids.shape
    groups = lax.axis_size("expert")
    capacity = 3 * tok_dev * top // (2 * groups)
    slots = groups * capacity
    live = jnp.arange(tok_dev, dtype=jnp.int32) < live_count[0]
    flat_expert = route_ids.reshape(-1)
    hits = (flat_expert[:, None] == jnp.arange(groups, dtype=jnp.int32)[None, :]).astype(jnp.int32)
    before = jnp.cumsum(hits, 0) - hits
    ranking = jnp.sum(before * hits, 1)
    target = flat_expert * capacity + ranking
    valid = jnp.repeat(live, top)
    chosen = (jnp.arange(slots, dtype=jnp.int32)[:, None] == target[None, :]) & valid[None, :]
    dispatch = jnp.sum(chosen.reshape(slots, tok_dev, top).astype(jnp.int32), 2).astype(
        jnp.bfloat16
    )
    gate_w = w_gate[0]
    up_w = w_up[0]
    down_w = w_down[0]
    out_width = down_w.shape[1]
    outgoing = jnp.dot(dispatch, tokens, preferred_element_type=jnp.float32).astype(jnp.bfloat16)
    outgoing = outgoing.reshape(groups, capacity, tokens.shape[1])
    piece = lax.all_to_all(outgoing, "expert", split_axis=0, concat_axis=0, tiled=True)
    piece = lax.all_gather(piece, "tensor", axis=2, tiled=True)
    sources, items, width = piece.shape
    count = sources * items
    rows = piece.reshape(count, width)
    gate = jnp.dot(rows, gate_w, preferred_element_type=jnp.float32)
    up = jnp.dot(rows, up_w, preferred_element_type=jnp.float32)
    result = jnp.dot(
        (jax.nn.silu(gate) * up).astype(jnp.bfloat16), down_w, preferred_element_type=jnp.float32
    )
    summed = lax.psum_scatter(
        result.reshape(sources, items, out_width), "tensor", scatter_dimension=2, tiled=True
    )
    results = summed.astype(jnp.bfloat16)
    returned = lax.all_to_all(results, "expert", split_axis=0, concat_axis=0, tiled=True)
    returned = returned.reshape(slots, returned.shape[2])
    picked = target.reshape(tok_dev, top)[owner_slot]
    weight = jnp.where(live[owner_slot][:, None], route_weight[owner_slot], jnp.float32(0.0))
    values = (
        returned[picked.reshape(-1)].reshape(tok_dev, top, returned.shape[1]).astype(jnp.float32)
    )
    mixed = jnp.sum(values * weight[:, :, None], 1)
    return mixed.astype(jnp.bfloat16)


def block_diagonal(picks):
    count, rows, cols = picks.shape
    same = jnp.eye(count, dtype=picks.dtype)
    return (picks[:, :, None, :] * same[:, None, :, None]).reshape(count * rows, count * cols)


def tree_body(tokens, w_gate, w_up, w_down, route_ids, route_weight, live_count, owner_slot):
    tok_dev, top = route_ids.shape
    width = tokens.shape[1]
    groups = lax.axis_size("expert")
    ring = groups // 4
    capacity = 3 * tok_dev * top // (2 * groups)
    bf16, f32 = jnp.bfloat16, jnp.float32
    me = lax.axis_index("expert")
    core = lax.axis_index("tensor")
    first = core == 0

    bits = ((2, 1), (1, 2))
    cells = [(e, c) for e in range(groups) for c in range(2)]

    def turn(places):
        return [(2 * e + c, 2 * ((e + 4 * places) % groups) + c) for e, c in cells]

    near = [(2 * e + c, 2 * (e ^ bits[c][0]) + c) for e, c in cells]
    far = [(2 * e + c, 2 * (e ^ bits[c][1]) + c) for e, c in cells]

    def swap(value):
        return lax.ppermute(value, "tensor", [(0, 1), (1, 0)])

    live = jnp.arange(tok_dev, dtype=jnp.int32) < live_count[0]
    named = jnp.where(live[:, None], route_ids, -1).astype(f32)
    table = jnp.concatenate([named, route_weight], 1).T
    blocks = [tokens]
    blocks.append(lax.ppermute(tokens, BOTH, turn(1)))
    beside = [lax.ppermute(tokens, BOTH, near)]
    table = jnp.stack([table, lax.ppermute(table, BOTH, near)])
    tables = [table] + [lax.ppermute(table, BOTH, turn(k)) for k in range(1, ring)]
    for _ in range(2, ring):
        blocks.append(lax.ppermute(blocks[-1], BOTH, turn(1)))
    for k in range(1, ring):
        beside.append(lax.ppermute(blocks[k], BOTH, near))
    far_bit = jnp.where(first, bits[0][1], bits[1][1])

    def picking(table, expert):
        match = (table[:, :top] == expert.astype(f32)).astype(f32)
        hit = jnp.sum(match, 1)
        earlier = jnp.tril(jnp.ones((tok_dev, tok_dev), f32), -1)
        rank = jnp.sum(hit[:, None, :] * earlier, -1)
        slot = jnp.arange(capacity, dtype=f32)
        pick = (rank[:, None, :] == slot[:, None]) & (hit[:, None, :] > 0)
        weight = jnp.sum(match * table[:, top:], 1)
        return pick, jnp.where(pick, weight[:, None, :], 0.0)

    gate_w, up_w, down_w = w_gate[0], w_up[0], w_down[0]
    own_down = lax.dynamic_slice_in_dim(down_w, core * width, width, 1)
    other_down = lax.dynamic_slice_in_dim(down_w, (1 - core) * width, width, 1)

    size = ring // CHUNKS
    count = size * capacity
    mine = [picking(t, me) for t in tables]
    theirs = [picking(t, me ^ far_bit) for t in tables]

    def select(picks, k, which):
        matrix = picks[k][0][which].astype(bf16)
        x = (blocks, beside)[which][k]
        return jnp.dot(matrix, x, preferred_element_type=f32).astype(bf16)

    got = [
        lax.ppermute(jnp.concatenate([select(theirs, k, 0), select(theirs, k, 1)], 0), BOTH, far)
        for k in range(ring)
    ]
    partial = []
    for chunk in range(CHUNKS):
        ks = slice(chunk * size, (chunk + 1) * size)
        kept = [jnp.concatenate([select(mine, k, w) for k in range(ring)[ks]], 0) for w in (0, 1)]
        came = [
            jnp.concatenate([g[w * capacity : (w + 1) * capacity] for g in got[ks]], 0)
            for w in (0, 1)
        ]
        a, b = jnp.where(first, came[0], kept[1]), jnp.where(first, kept[1], came[0])
        rows = jnp.concatenate([kept[0], a, b, came[1]], 0)
        peer = swap(rows)
        full = jnp.concatenate(
            [jnp.where(first, rows, peer), jnp.where(first, peer, rows)], 1
        )
        gate = jnp.dot(full, gate_w, preferred_element_type=f32)
        up = jnp.dot(full, up_w, preferred_element_type=f32)
        hidden = (jax.nn.silu(gate) * up).astype(bf16)
        there = jnp.dot(hidden, other_down, preferred_element_type=f32).astype(bf16)
        here = jnp.dot(hidden, own_down, preferred_element_type=f32)
        out = (here + swap(there).astype(f32)).astype(bf16).reshape(4, count, width)
        one = jnp.where(first, out[1], out[2])
        back = lax.ppermute(jnp.concatenate([one, out[3]], 0), BOTH, far)
        near_own = jnp.where(first, out[2], out[1])

        def spread(which, own, remote):
            exact = jnp.concatenate(
                [
                    block_diagonal(jnp.stack([p[1][which] for p in picks[ks]]))
                    for picks in (mine, theirs)
                ],
                0,
            )
            high = exact.astype(bf16)
            low = (exact - high.astype(f32)).astype(bf16)
            values = jnp.concatenate([own, remote], 0)
            return sum(
                lax.dot_general(
                    part, values, (((0,), (0,)), ((), ())), preferred_element_type=f32
                )
                for part in (high, low)
            )

        beside_sum = spread(1, near_own, back[count:]).astype(bf16)
        arrived = jnp.concatenate(
            [
                lax.ppermute(beside_sum[k * tok_dev : (k + 1) * tok_dev], BOTH, near)
                for k in range(size)
            ],
            0,
        )
        total = spread(0, out[0], back[:count]) + arrived.astype(f32)
        partial += [total[k * tok_dev : (k + 1) * tok_dev] for k in range(size)]

    running = partial[1]
    for k in range(2, ring + 1):
        running = partial[k % ring] + lax.ppermute(running.astype(bf16), BOTH, turn(1)).astype(f32)
    return running.astype(bf16)[owner_slot]


def solution(mesh):
    groups, cores = mesh.shape["expert"], mesh.shape["tensor"]

    def body(tokens, *rest):
        tok_dev, top = rest[3].shape
        capacity = 3 * tok_dev * top // (2 * groups)
        blocks_pay = cores == 2 and groups % 8 == 0 and tok_dev <= 2 * capacity
        return (tree_body if blocks_pay else exchange_body)(tokens, *rest)

    placed = (
        P("expert", "tensor"),
        P("expert", None, "tensor"),
        P("expert", None, "tensor"),
        P("expert", "tensor", None),
        P("expert", None),
        P("expert", None),
        P("expert"),
        P("expert"),
    )
    return jax.shard_map(
        body, mesh=mesh, in_specs=placed, out_specs=P("expert", "tensor"), check_vma=False
    )
```

```python
import functools

import jax
import jax.numpy as jnp
import numpy as np
from jax import lax
from jax.experimental import pallas as pl
from jax.experimental.pallas import tpu as pltpu
from jax.sharding import PartitionSpec as P

BF16, F32 = jnp.bfloat16, jnp.float32
BOTH = ("expert", "tensor")


def exchange_body(tokens, w_gate, w_up, w_down, route_ids, route_weight, live_count, owner_slot):
    tok_dev, top = route_ids.shape
    groups = lax.axis_size("expert")
    capacity = 3 * tok_dev * top // (2 * groups)
    slots = groups * capacity
    live = jnp.arange(tok_dev, dtype=jnp.int32) < live_count[0]
    flat_expert = route_ids.reshape(-1)
    hits = (flat_expert[:, None] == jnp.arange(groups, dtype=jnp.int32)[None, :]).astype(jnp.int32)
    before = jnp.cumsum(hits, 0) - hits
    ranking = jnp.sum(before * hits, 1)
    target = flat_expert * capacity + ranking
    valid = jnp.repeat(live, top)
    chosen = (jnp.arange(slots, dtype=jnp.int32)[:, None] == target[None, :]) & valid[None, :]
    dispatch = jnp.sum(chosen.reshape(slots, tok_dev, top).astype(jnp.int32), 2).astype(
        jnp.bfloat16
    )
    gate_w = w_gate[0]
    up_w = w_up[0]
    down_w = w_down[0]
    out_width = down_w.shape[1]
    outgoing = jnp.dot(dispatch, tokens, preferred_element_type=jnp.float32).astype(jnp.bfloat16)
    outgoing = outgoing.reshape(groups, capacity, tokens.shape[1])
    piece = lax.all_to_all(outgoing, "expert", split_axis=0, concat_axis=0, tiled=True)
    piece = lax.all_gather(piece, "tensor", axis=2, tiled=True)
    sources, items, width = piece.shape
    count = sources * items
    rows = piece.reshape(count, width)
    gate = jnp.dot(rows, gate_w, preferred_element_type=jnp.float32)
    up = jnp.dot(rows, up_w, preferred_element_type=jnp.float32)
    result = jnp.dot(
        (jax.nn.silu(gate) * up).astype(jnp.bfloat16), down_w, preferred_element_type=jnp.float32
    )
    summed = lax.psum_scatter(
        result.reshape(sources, items, out_width), "tensor", scatter_dimension=2, tiled=True
    )
    results = summed.astype(jnp.bfloat16)
    returned = lax.all_to_all(results, "expert", split_axis=0, concat_axis=0, tiled=True)
    returned = returned.reshape(slots, returned.shape[2])
    picked = target.reshape(tok_dev, top)[owner_slot]
    weight = jnp.where(live[owner_slot][:, None], route_weight[owner_slot], jnp.float32(0.0))
    values = (
        returned[picked.reshape(-1)].reshape(tok_dev, top, returned.shape[1]).astype(jnp.float32)
    )
    mixed = jnp.sum(values * weight[:, :, None], 1)
    return mixed.astype(jnp.bfloat16)


def call(kernel, outs, scalars, operands, grid, in_specs, out_specs, scratch=(), flops=0):
    moved = sum(x.size * x.dtype.itemsize for x in operands)
    return pl.pallas_call(
        kernel,
        out_shape=outs,
        grid_spec=pltpu.PrefetchScalarGridSpec(
            num_scalar_prefetch=1,
            grid=grid,
            in_specs=in_specs,
            out_specs=out_specs,
            scratch_shapes=scratch,
        ),
        compiler_params=pltpu.CompilerParams(vmem_limit_bytes=2**22),
        cost_estimate=pl.CostEstimate(flops=flops, bytes_accessed=moved, transcendentals=0),
    )(scalars, *operands)


def whole(x):
    return pl.BlockSpec(x.shape, lambda i, s: (0,) * len(x.shape))


def iota(shape, dim):
    return lax.broadcasted_iota(jnp.int32, shape, dim)


def targets(table, expert, top, capacity):
    lanes = table.shape[1]
    match = table[:top].astype(jnp.int32) == expert
    hit = jnp.sum(match.astype(F32), 0, keepdims=True)
    weight = jnp.sum(jnp.where(match, table[8 : 8 + top], 0.0), 0, keepdims=True)
    row, col = iota((lanes, lanes), 0), iota((lanes, lanes), 1)
    half = lanes // 2
    earlier = (row < col) & ((row >= half) == (col >= half))
    rank = jnp.dot(
        jnp.broadcast_to(hit, (8, lanes)).astype(BF16),
        earlier.astype(F32).astype(BF16),
        preferred_element_type=F32,
    )[:1]
    second = (iota((1, lanes), 1) >= half).astype(jnp.int32)
    slot = rank.astype(jnp.int32) + capacity * second
    return jnp.where(hit > 0, slot, -1), weight


def routing_kernel(top, capacity, s_ref, table_ref, send_ref, keep_ref, high_ref, low_ref):
    table = table_ref[...]
    lanes = table.shape[1]
    half, count = lanes // 2, 2 * capacity
    depth = -(-2 * count // 128) * 128
    exact = jnp.zeros((depth, lanes), F32)
    for which, out_ref in ((0, keep_ref), (1, send_ref)):
        slot, weight = targets(table, s_ref[which], top, capacity)
        out_ref[...] = (iota((count, lanes), 0) == slot).astype(F32).astype(BF16)
        slot = jnp.where(slot >= 0, slot + which * count, -1)
        exact += jnp.where(iota((depth, lanes), 0) == slot, weight, 0.0)
    owner = table[top : top + 1].astype(jnp.int32)
    owner = owner + half * (iota((1, lanes), 1) >= half).astype(jnp.int32)
    place = (iota((lanes, lanes), 0) == owner).astype(F32).T.astype(BF16)
    exact = exact.T
    high = exact.astype(BF16)
    low = (exact - high.astype(F32)).astype(BF16)
    for part, out_ref in ((high, high_ref), (low, low_ref)):
        out_ref[...] = jnp.dot(place, part, preferred_element_type=F32).astype(BF16)


def routing(scalars, top, capacity, table):
    lanes = table.shape[1]
    depth = -(-4 * capacity // 128) * 128
    outs = [jax.ShapeDtypeStruct((2 * capacity, lanes), BF16)] * 2
    outs += [jax.ShapeDtypeStruct((lanes, depth), BF16)] * 2
    return call(
        functools.partial(routing_kernel, top, capacity),
        outs,
        scalars,
        [table],
        (1,),
        [whole(table)],
        [whole(x) for x in outs],
        flops=2**22,
    )


def crossing(capacity, size):
    count = 2 * capacity
    source = np.arange(2 * count * size)
    for p in range(size):
        kept, came = p * count + capacity, (size + p) * count
        source[kept : kept + capacity] = np.arange(came, came + capacity)
        source[came : came + capacity] = np.arange(kept, kept + capacity)
    return jnp.asarray(source[:, None] == np.arange(2 * count * size)[None, :], BF16)


def dot(a, b, kind=F32):
    return jnp.dot(a, b, preferred_element_type=F32).astype(kind)


def tree_body(tokens, w_gate, w_up, w_down, route_ids, route_weight, live_count, owner_slot):
    tok_dev, top = route_ids.shape
    width = tokens.shape[1]
    groups = lax.axis_size("expert")
    ring = groups // 4
    capacity = 3 * tok_dev * top // (2 * groups)
    count = 2 * capacity
    me = lax.axis_index("expert")
    core = lax.axis_index("tensor")

    bits = ((2, 1), (1, 2))
    cells = [(e, c) for e in range(groups) for c in range(2)]

    def turn(places):
        return [(2 * e + c, 2 * ((e + 4 * places) % groups) + c) for e, c in cells]

    near = [(2 * e + c, 2 * (e ^ bits[c][0]) + c) for e, c in cells]
    far = [(2 * e + c, 2 * (e ^ bits[c][1]) + c) for e, c in cells]
    scalars = jnp.stack([me, me ^ jnp.where(core == 0, bits[0][1], bits[1][1]), core])

    def send(name, value, pairs):
        with jax.named_scope(name):
            return lax.ppermute(value, BOTH, pairs)

    def swap(value):
        return lax.ppermute(value, "tensor", [(0, 1), (1, 0)])

    def after(value, *events):
        return lax.optimization_barrier((value, *events))[0]

    live = jnp.arange(tok_dev, dtype=jnp.int32) < live_count[0]
    table = jnp.concatenate(
        [
            jnp.where(live[:, None], route_ids, -1).astype(F32),
            owner_slot.astype(F32)[:, None],
            jnp.zeros((tok_dev, 7 - top), F32),
            route_weight,
            jnp.zeros((tok_dev, 8 - top), F32),
        ],
        1,
    ).T
    def halves(w, dim):
        return [lax.dynamic_slice_in_dim(w[0], c * width, width, dim) for c in (core, 1 - core)]

    gates, ups, downs = halves(w_gate, 0), halves(w_up, 0), halves(w_down, 1)
    blocks, tables, beside, made, sent, got = {}, {}, {}, {}, {}, {}
    arriving, state, back, partial, own_sum, near_sum = {}, {}, {}, {}, {}, {}
    last = []

    def then(value):
        return after(value, *last)

    def done(value):
        last[:] = [value]
        return value

    def pick(matrix, k):
        a, b = matrix[:, :tok_dev], matrix[:, tok_dev:]
        return (dot(a, blocks[k]) + dot(b, beside[k])).astype(BF16)

    def spread(k):
        blocks[k] = done(then(arriving[k])) if k else tokens
        if k + 1 < ring:
            arriving[k + 1] = send(f"ring{k + 1}", blocks[k], turn(1))
        beside[k] = send(f"near{k}", blocks[k], near)
        if k:
            tables[k] = after(tables[k], blocks[k])
        else:
            tables[0] = jnp.concatenate([table, send("tnear", table, near)], 1)
        if k + 1 < ring:
            tables[k + 1] = send(f"turn{k + 1}", tables[k], turn(1))

    def route(k):
        made[k] = routing(scalars, top, capacity, then(tables[k]))
        done(made[k][0])

    def select(k):
        beside[k] = then(beside[k])
        sent[k] = done(pick(made[k][0], k))
        got[k] = send(f"far{k}", sent[k], far)

    def rows(ks):
        cross = crossing(capacity, len(ks))
        mine = jnp.concatenate([pick(made[k][1], k) for k in ks] + [then(got[k]) for k in ks])
        state[ks[0]] = [mine, swap(done(dot(cross, mine, BF16))), cross]

    def own_half(ks):
        mine = then(state[ks[0]][0])
        state[ks[0]][0] = done(lax.optimization_barrier((dot(mine, gates[0]), dot(mine, ups[0]))))

    def peer_half(ks):
        (gate, up), peer, cross = state[ks[0]]
        peer = then(peer)
        gate += dot(peer, gates[1])
        up += dot(peer, ups[1])
        hidden = after((gate / (1.0 + jnp.exp(-gate)) * up).astype(BF16))
        crossed = after(dot(cross, hidden, BF16))
        state[ks[0]] = [hidden, swap(done(dot(crossed, downs[1], BF16)))]

    def finish(ks):
        hidden, there = state[ks[0]]
        here = dot(hidden, downs[0])
        out = (here + then(there).astype(F32)).astype(BF16)
        came = [out[(len(ks) + p) * count : (len(ks) + p + 1) * count] for p in range(len(ks))]
        came = done(lax.optimization_barrier(tuple(came)))
        for p, k in enumerate(ks):
            back[k] = out[p * count : (p + 1) * count], send(f"back{k}", came[p], far)

    def merge(k):
        high, low = made[k][2:]
        stay, came = back[k]
        came = then(came)

        def add(matrix):
            return dot(matrix[:, :count], stay) + dot(matrix[:, count : 2 * count], came)

        total = done((add(high[tok_dev:]) + add(low[tok_dev:])).astype(BF16))
        near_sum[k] = send(f"sum{k}", total, near)
        own_sum[k] = add(high[:tok_dev]) + add(low[:tok_dev])

    def pass_on(k):
        total = own_sum[k % ring] + then(near_sum[k % ring]).astype(F32)
        if k > 1:
            total += partial[k - 1].astype(F32)
        total = done(total.astype(BF16))
        partial[k] = send(f"add{k + 1}", total, turn(1)) if k < ring else total

    passes = {k: [k] for k in range(1, ring - 1)}
    passes[ring - 1] = [ring - 1, 0]
    plan = [(spread, 0), (route, 0), (spread, 1), (select, 0), (route, 1), (select, 1), (spread, 2)]
    for k, ks in passes.items():
        plan += [(rows, ks), (own_half, ks)]
        if k + 1 < ring:
            plan += [(route, k + 1), (select, k + 1)]
        if k > 2:
            plan += [(pass_on, k - 2)]
        plan += [(peer_half, ks)]
        if k + 2 < ring:
            plan += [(spread, k + 2)]
        if k > 1:
            plan += [(merge, k - 1)]
        plan += [(finish, ks)]
    plan += [(pass_on, ring - 2), (merge, ring - 1), (pass_on, ring - 1), (merge, 0)]
    for stage, which in plan + [(pass_on, ring)]:
        stage(which)
    return partial[ring]


def solution(mesh):
    groups, cores = mesh.shape["expert"], mesh.shape["tensor"]

    def body(tokens, *rest):
        tok_dev, top = rest[3].shape
        capacity = 3 * tok_dev * top // (2 * groups)
        blocks_pay = cores == 2 and groups % 8 == 0 and tok_dev <= 2 * capacity
        return (tree_body if blocks_pay else exchange_body)(tokens, *rest)

    placed = (
        P("expert", "tensor"),
        P("expert", None, "tensor"),
        P("expert", None, "tensor"),
        P("expert", "tensor", None),
        P("expert", None),
        P("expert", None),
        P("expert"),
        P("expert"),
    )
    return jax.shard_map(
        body, mesh=mesh, in_specs=placed, out_specs=P("expert", "tensor"), check_vma=False
    )
```

```python
import functools

import jax
import jax.numpy as jnp
import numpy as np
from jax import lax
from jax.experimental import pallas as pl
from jax.experimental.pallas import tpu as pltpu
from jax.sharding import PartitionSpec as P

BF16, F32 = jnp.bfloat16, jnp.float32
BOTH = ("expert", "tensor")


def exchange_body(tokens, w_gate, w_up, w_down, route_ids, route_weight, live_count, owner_slot):
    tok_dev, top = route_ids.shape
    groups = lax.axis_size("expert")
    capacity = 3 * tok_dev * top // (2 * groups)
    slots = groups * capacity
    live = jnp.arange(tok_dev, dtype=jnp.int32) < live_count[0]
    flat_expert = route_ids.reshape(-1)
    hits = (flat_expert[:, None] == jnp.arange(groups, dtype=jnp.int32)[None, :]).astype(jnp.int32)
    before = jnp.cumsum(hits, 0) - hits
    ranking = jnp.sum(before * hits, 1)
    target = flat_expert * capacity + ranking
    valid = jnp.repeat(live, top)
    chosen = (jnp.arange(slots, dtype=jnp.int32)[:, None] == target[None, :]) & valid[None, :]
    dispatch = jnp.sum(chosen.reshape(slots, tok_dev, top).astype(jnp.int32), 2).astype(
        jnp.bfloat16
    )
    gate_w = w_gate[0]
    up_w = w_up[0]
    down_w = w_down[0]
    out_width = down_w.shape[1]
    outgoing = jnp.dot(dispatch, tokens, preferred_element_type=jnp.float32).astype(jnp.bfloat16)
    outgoing = outgoing.reshape(groups, capacity, tokens.shape[1])
    piece = lax.all_to_all(outgoing, "expert", split_axis=0, concat_axis=0, tiled=True)
    piece = lax.all_gather(piece, "tensor", axis=2, tiled=True)
    sources, items, width = piece.shape
    count = sources * items
    rows = piece.reshape(count, width)
    gate = jnp.dot(rows, gate_w, preferred_element_type=jnp.float32)
    up = jnp.dot(rows, up_w, preferred_element_type=jnp.float32)
    result = jnp.dot(
        (jax.nn.silu(gate) * up).astype(jnp.bfloat16), down_w, preferred_element_type=jnp.float32
    )
    summed = lax.psum_scatter(
        result.reshape(sources, items, out_width), "tensor", scatter_dimension=2, tiled=True
    )
    results = summed.astype(jnp.bfloat16)
    returned = lax.all_to_all(results, "expert", split_axis=0, concat_axis=0, tiled=True)
    returned = returned.reshape(slots, returned.shape[2])
    picked = target.reshape(tok_dev, top)[owner_slot]
    weight = jnp.where(live[owner_slot][:, None], route_weight[owner_slot], jnp.float32(0.0))
    values = (
        returned[picked.reshape(-1)].reshape(tok_dev, top, returned.shape[1]).astype(jnp.float32)
    )
    mixed = jnp.sum(values * weight[:, :, None], 1)
    return mixed.astype(jnp.bfloat16)


def call(kernel, outs, scalars, operands, grid, in_specs, out_specs, scratch=(), flops=0):
    moved = sum(x.size * x.dtype.itemsize for x in operands)
    return pl.pallas_call(
        kernel,
        out_shape=outs,
        grid_spec=pltpu.PrefetchScalarGridSpec(
            num_scalar_prefetch=1,
            grid=grid,
            in_specs=in_specs,
            out_specs=out_specs,
            scratch_shapes=scratch,
        ),
        compiler_params=pltpu.CompilerParams(vmem_limit_bytes=2**22),
        cost_estimate=pl.CostEstimate(flops=flops, bytes_accessed=moved, transcendentals=0),
    )(scalars, *operands)


def whole(x):
    return pl.BlockSpec(x.shape, lambda i, s: (0,) * len(x.shape))


def iota(shape, dim):
    return lax.broadcasted_iota(jnp.int32, shape, dim)


def targets(table, expert, top, capacity):
    lanes = table.shape[1]
    match = table[:top].astype(jnp.int32) == expert
    hit = jnp.sum(match.astype(F32), 0, keepdims=True)
    weight = jnp.sum(jnp.where(match, table[8 : 8 + top], 0.0), 0, keepdims=True)
    row, col = iota((lanes, lanes), 0), iota((lanes, lanes), 1)
    half = lanes // 2
    earlier = (row < col) & ((row >= half) == (col >= half))
    rank = jnp.dot(
        jnp.broadcast_to(hit, (8, lanes)).astype(BF16),
        earlier.astype(F32).astype(BF16),
        preferred_element_type=F32,
    )[:1]
    second = (iota((1, lanes), 1) >= half).astype(jnp.int32)
    slot = rank.astype(jnp.int32) + capacity * second
    return jnp.where(hit > 0, slot, -1), weight


def routing_kernel(top, capacity, s_ref, table_ref, send_ref, keep_ref, high_ref, low_ref):
    table = table_ref[...]
    lanes = table.shape[1]
    half, count = lanes // 2, 2 * capacity
    depth = -(-2 * count // 128) * 128
    exact = jnp.zeros((depth, lanes), F32)
    for which, out_ref in ((0, keep_ref), (1, send_ref)):
        slot, weight = targets(table, s_ref[which], top, capacity)
        out_ref[...] = (iota((count, lanes), 0) == slot).astype(F32).astype(BF16)
        slot = jnp.where(slot >= 0, slot + which * count, -1)
        exact += jnp.where(iota((depth, lanes), 0) == slot, weight, 0.0)
    owner = table[top : top + 1].astype(jnp.int32)
    owner = owner + half * (iota((1, lanes), 1) >= half).astype(jnp.int32)
    place = (iota((lanes, lanes), 0) == owner).astype(F32).T.astype(BF16)
    exact = exact.T
    high = exact.astype(BF16)
    low = (exact - high.astype(F32)).astype(BF16)
    for part, out_ref in ((high, high_ref), (low, low_ref)):
        out_ref[...] = jnp.dot(place, part, preferred_element_type=F32).astype(BF16)


def routing(scalars, top, capacity, table):
    lanes = table.shape[1]
    depth = -(-4 * capacity // 128) * 128
    outs = [jax.ShapeDtypeStruct((2 * capacity, lanes), BF16)] * 2
    outs += [jax.ShapeDtypeStruct((lanes, depth), BF16)] * 2
    return call(
        functools.partial(routing_kernel, top, capacity),
        outs,
        scalars,
        [table],
        (1,),
        [whole(table)],
        [whole(x) for x in outs],
        flops=2**22,
    )


def crossing(capacity, size):
    count = 2 * capacity
    source = np.arange(2 * count * size)
    for p in range(size):
        kept, came = p * count + capacity, (size + p) * count
        source[kept : kept + capacity] = np.arange(came, came + capacity)
        source[came : came + capacity] = np.arange(kept, kept + capacity)
    return jnp.asarray(source[:, None] == np.arange(2 * count * size)[None, :], BF16)


def dot(a, b, kind=F32):
    return jnp.dot(a, b, preferred_element_type=F32).astype(kind)


def stage_order(ring):
    end = ring - 1
    plan = [("spread", 0), ("spread", 1), ("route", 1), ("select", 1), ("spread", 2)]
    plan += [("route", 0), ("select", 0)]
    for k in range(1, ring):
        plan += [("rows", [k]), ("own_half", [k])]
        if k < end:
            plan += [("route", k + 1), ("select", k + 1)]
        if k > 1:
            plan += [("merge", k - 1)]
        plan += [("peer_half", [k])]
        if k + 1 < end:
            plan += [("spread", k + 2)]
        plan += [("finish", [k])]
        if 1 < k < end:
            plan += [("pass_on", k - 1)]
    plan += [("rows", [0]), ("own_half", [0]), ("pass_on", end - 1), ("peer_half", [0])]
    plan += [("merge", end), ("finish", [0]), ("pass_on", end), ("merge", 0)]
    return plan + [("pass_on", ring)]


def tree_body(tokens, w_gate, w_up, w_down, route_ids, route_weight, live_count, owner_slot):
    tok_dev, top = route_ids.shape
    width = tokens.shape[1]
    groups = lax.axis_size("expert")
    ring = groups // 4
    capacity = 3 * tok_dev * top // (2 * groups)
    count = 2 * capacity
    me = lax.axis_index("expert")
    core = lax.axis_index("tensor")

    bits = ((2, 1), (1, 2))
    cells = [(e, c) for e in range(groups) for c in range(2)]

    def turn(places):
        return [(2 * e + c, 2 * ((e + 4 * places) % groups) + c) for e, c in cells]

    near = [(2 * e + c, 2 * (e ^ bits[c][0]) + c) for e, c in cells]
    far = [(2 * e + c, 2 * (e ^ bits[c][1]) + c) for e, c in cells]
    scalars = jnp.stack([me, me ^ jnp.where(core == 0, bits[0][1], bits[1][1]), core])

    def send(value, pairs):
        return lax.ppermute(value, BOTH, pairs)

    def swap(value):
        return send(value, [(2 * e + c, 2 * e + 1 - c) for e, c in cells])

    def after(value, *events):
        return lax.optimization_barrier((value, *events))[0]

    live = jnp.arange(tok_dev, dtype=jnp.int32) < live_count[0]
    table = jnp.concatenate(
        [
            jnp.where(live[:, None], route_ids, -1).astype(F32),
            owner_slot.astype(F32)[:, None],
            jnp.zeros((tok_dev, 7 - top), F32),
            route_weight,
            jnp.zeros((tok_dev, 8 - top), F32),
        ],
        1,
    ).T

    def halves(w, dim):
        return [lax.dynamic_slice_in_dim(w[0], c * width, width, dim) for c in (core, 1 - core)]

    gates, ups, downs = halves(w_gate, 0), halves(w_up, 0), halves(w_down, 1)
    blocks, tables, beside, made, sent, kept, got = {}, {}, {}, {}, {}, {}, {}
    arriving, state, back, partial, own_sum, near_sum = {}, {}, {}, {}, {}, {}
    last = []

    def then(value):
        return after(value, *last)

    def done(value):
        last[:] = [value]
        return value

    def pick(matrix, k):
        a, b = matrix[:, :tok_dev], matrix[:, tok_dev:]
        return (dot(a, blocks[k]) + dot(b, beside[k])).astype(BF16)

    def spread(k):
        blocks[k] = done(then(arriving[k])) if k else tokens
        if k + 1 < ring:
            arriving[k + 1] = send(blocks[k], turn(1))
        beside[k] = send(blocks[k], near)
        if k:
            tables[k] = after(tables[k], blocks[k])
        else:
            tables[0] = jnp.concatenate([table, send(table, near)], 1)
        if k + 1 < ring:
            tables[k + 1] = send(tables[k], turn(1))

    def route(k):
        made[k] = routing(scalars, top, capacity, then(tables[k]))
        done(made[k][0])

    def select(k):
        beside[k] = then(beside[k])
        kept[k] = done(pick(made[k][1], k))
        sent[k] = done(pick(then(made[k][0]), k))
        got[k] = send(sent[k], far)

    def rows(ks):
        cross = crossing(capacity, len(ks))
        mine = jnp.concatenate([kept[k] for k in ks] + [then(got[k]) for k in ks])
        state[ks[0]] = [mine, swap(done(dot(cross, mine, BF16))), cross]

    def own_half(ks):
        mine = then(state[ks[0]][0])
        state[ks[0]][0] = done(lax.optimization_barrier((dot(mine, gates[0]), dot(mine, ups[0]))))

    def peer_half(ks):
        (gate, up), peer, cross = state[ks[0]]
        peer = then(peer)
        gate += dot(peer, gates[1])
        up += dot(peer, ups[1])
        hidden = after((gate / (1.0 + jnp.exp(-gate)) * up).astype(BF16))
        crossed = after(dot(cross, hidden, BF16))
        state[ks[0]] = [hidden, swap(done(dot(crossed, downs[1], BF16)))]

    def finish(ks):
        hidden, there = state[ks[0]]
        here = dot(hidden, downs[0])
        out = (here + then(there).astype(F32)).astype(BF16)
        came = [out[(len(ks) + p) * count : (len(ks) + p + 1) * count] for p in range(len(ks))]
        came = done(lax.optimization_barrier(tuple(came)))
        for p, k in enumerate(ks):
            back[k] = out[p * count : (p + 1) * count], send(came[p], far)

    def merge(k):
        high, low = made[k][2:]
        stay, came = back[k]
        came = then(came)

        def add(matrix):
            return dot(matrix[:, :count], stay) + dot(matrix[:, count : 2 * count], came)

        total = done((add(high[tok_dev:]) + add(low[tok_dev:])).astype(BF16))
        near_sum[k] = send(total, near)
        own_sum[k] = add(high[:tok_dev]) + add(low[:tok_dev])

    def pass_on(k):
        total = own_sum[k % ring] + then(near_sum[k % ring]).astype(F32)
        if k > 1:
            total = after(total) + partial[k - 1].astype(F32)
        total = done(total.astype(BF16))
        partial[k] = send(total, turn(1)) if k < ring else total

    stages = dict(
        spread=spread,
        route=route,
        select=select,
        rows=rows,
        own_half=own_half,
        peer_half=peer_half,
        finish=finish,
        merge=merge,
        pass_on=pass_on,
    )
    for stage, which in stage_order(ring):
        stages[stage](which)
    return partial[ring]


def solution(mesh):
    groups, cores = mesh.shape["expert"], mesh.shape["tensor"]

    def body(tokens, *rest):
        tok_dev, top = rest[3].shape
        capacity = 3 * tok_dev * top // (2 * groups)
        blocks_pay = cores == 2 and groups % 8 == 0 and tok_dev <= 2 * capacity
        return (tree_body if blocks_pay else exchange_body)(tokens, *rest)

    placed = (
        P("expert", "tensor"),
        P("expert", None, "tensor"),
        P("expert", None, "tensor"),
        P("expert", "tensor", None),
        P("expert", None),
        P("expert", None),
        P("expert"),
        P("expert"),
    )
    return jax.shard_map(
        body, mesh=mesh, in_specs=placed, out_specs=P("expert", "tensor"), check_vma=False
    )
```
